32 devices in a mesh: pop: 16 (over z, y, core), fsdp: 2 (over x).
Axes of the slice: x: 2, y: 2, z: 4, core: 2. Of those that a mesh axis runs over, the one named last changes fastest.
Arguments:
- tokens: bfloat16 [14336, 4096], P('pop', 'fsdp'), may hold values from -6 to 6
- up_weight: bfloat16 [4096, 14336], P('pop', 'fsdp'), may hold values from -0.09375 to 0.09375
- a_bank: bfloat16 [1024, 4096], P(None, 'pop'), may hold values from -6 to 6
- b_bank: bfloat16 [1024, 14336], P(None, 'fsdp'), may hold values from -6 to 6
- factor_index: int32 [32, 4], replicated, may hold values from 0 to 1023
- mirror: int32 [32], P('pop'), may hold values 0 or 1
- rewards: int32 [32], P('pop'), may hold values from -8 to 7
Outputs:
- hidden: bfloat16 [14336, 14336], P('pop', 'fsdp')
- update: float32 [4096, 14336], P('pop', 'fsdp')
The draws below stay inside these ranges and needn't reach their ends.
All inputs are finite; a program needn't handle non-finite values. No bound on the sum of `mirror` on one device may be relied on, other than what follows from the above.
Results may differ from the reference program's by a relative error of at most 0.001.
Values may be sent and summed in bfloat16 or wider, within the bound.
No kernel may reach another device: no remote copies, remote signals or barrier semaphores. Data moves between devices by JAX's collectives and lax.ppermute only.
A program may use at most 192 MiB of HBM per device.

```python
import math
import jax
import jax.numpy as jnp
from jax import lax

D = 4096
FF = 14336
RANK = 4
SEQ = 448
BANK = 1024
MEMBERS = 32
TOKENS = 14336


def place_ends(entries, stream_key, smallest, largest):
    dims = entries.shape
    index_at = [jax.random.randint(jax.random.fold_in(stream_key, axis), (), 0, dims[axis]) for axis in range(len(dims))]
    entries = entries.at[tuple(index_at)].set(smallest)
    longest = dims.index(max(dims))
    index_at[longest] = (index_at[longest] + 1) % dims[longest]
    return entries.at[tuple(index_at)].set(largest)


def block_scale(key, extent, split, least, top_value):
    gain = 1.0
    for dim, blocks in split:
        steps = jax.random.uniform(jax.random.fold_in(jax.random.fold_in(key, 6), dim), (blocks,), jnp.float32, least / len(split), top_value / len(split))
        gain = gain * jnp.repeat(jnp.exp(steps), extent[dim] // blocks).reshape((-1,) + (1,) * (len(extent) - 1 - dim))
    return gain


def normal_values(stream_key, extent, deviation, limit, shards=(), held_as=jnp.bfloat16):
    result = jax.random.normal(stream_key, extent, jnp.float32) * deviation
    if len(shards) > 0:
        result = block_scale(stream_key, extent, shards, -0.22, 0.18) * result
    return jnp.clip(result, min=-limit, max=limit).astype(held_as)


def setup_inputs(seed: int = 0) -> dict:
    key_list = jax.random.split(jax.random.key(seed), 8)
    return {
        "tokens": normal_values(key_list[0], (TOKENS, D), 1.0, 6.0, ((0, 16), (1, 2))),
        "up_weight": normal_values(key_list[1], (D, FF), D ** -0.5, 0.09375, ((0, 16), (1, 2))),
        "a_bank": normal_values(key_list[2], (BANK, D), 1.0, 6.0, ((1, 16),)),
        "b_bank": normal_values(key_list[3], (BANK, FF), 1.0, 6.0, ((1, 2),)),
        "factor_index": place_ends(jax.random.randint(key_list[4], (MEMBERS, RANK), 0, BANK), jax.random.fold_in(key_list[4], 1), 0, BANK - 1).astype(jnp.int32),
        "mirror": place_ends((jax.random.randint(key_list[5], (MEMBERS,), 0, 2) < 1).astype(jnp.int32), jax.random.fold_in(key_list[5], 1), 0, 1),
        "rewards": place_ends(jax.random.randint(key_list[6], (MEMBERS,), -8, 8), jax.random.fold_in(key_list[6], 1), -8, 7).astype(jnp.int32),
    }


noise_scale = 0.5

def shaped_weights(rewards, mirror):
    members_all = rewards.shape[0]
    member_ids = jnp.arange(members_all)
    beaten = rewards[None, :] < rewards[:, None]
    level_tie = (rewards[None, :] == rewards[:, None]) & (member_ids[None, :] < member_ids[:, None])
    standing = lax.optimization_barrier(jnp.sum((beaten | level_tie).astype(jnp.int32), axis=1))
    signed = (2 * mirror - 1).astype(jnp.float32)
    shaped = 2.0 * standing.astype(jnp.float32) / (members_all - 1) - 1.0
    return shaped * signed / math.sqrt(members_all * RANK)

def reference(tokens, up_weight, a_bank, b_bank, factor_index, mirror, rewards):
    members_all = factor_index.shape[0]
    factors_a = a_bank[factor_index]
    factors_b = b_bank[factor_index]
    signed = (2 * mirror - 1).astype(jnp.float32)
    scaling = noise_scale / math.sqrt(D * RANK)
    sequences = tokens.reshape(members_all, SEQ, D)

    def one_member(inputs):
        row_block, rows_a, rows_b, sign_one = inputs
        dense_out = jnp.dot(row_block, up_weight, preferred_element_type=jnp.float32)
        projected = jnp.dot(row_block, rows_a.T, preferred_element_type=jnp.float32)
        perturbed = jnp.dot(projected * (scaling * sign_one), rows_b.astype(jnp.float32), precision=lax.Precision.HIGHEST)
        return (dense_out + perturbed).astype(jnp.bfloat16)
    hidden = lax.map(one_member, (sequences, factors_a, factors_b, signed)).reshape(members_all * SEQ, FF)
    weighting = shaped_weights(rewards, mirror)
    spread = jnp.repeat(weighting, RANK)
    flat_a = factors_a.reshape(members_all * RANK, D).astype(jnp.float32)
    flat_b = factors_b.reshape(members_all * RANK, FF).astype(jnp.float32)
    update = jnp.dot(flat_a.T, spread[:, None] * flat_b, precision=lax.Precision.HIGHEST)
    return (hidden, update)
```

```python
import math

import jax
import jax.numpy as jnp
from jax import lax
from jax.experimental import pallas as pl
from jax.experimental.pallas import tpu as pltpu
from jax.sharding import PartitionSpec as P


D = 4096
RANK = 4
SEQ = 448
LANES = 128
LATE_SHARE = 7


noise_scale = 0.5


def shaped_weights(rewards, mirror):
    members_all = rewards.shape[0]
    member_ids = jnp.arange(members_all)
    beaten = rewards[None, :] < rewards[:, None]
    level_tie = (rewards[None, :] == rewards[:, None]) & (member_ids[None, :] < member_ids[:, None])
    standing = jnp.sum((beaten | level_tie).astype(jnp.int32), axis=1)
    signed = (2 * mirror - 1).astype(jnp.float32)
    shaped = 2.0 * standing.astype(jnp.float32) / (members_all - 1) - 1.0
    return shaped * signed / math.sqrt(members_all * RANK)


def whole_rows(tokens, parts):
    me = lax.axis_index("fsdp")
    width = tokens.shape[1]
    full = jnp.zeros((tokens.shape[0], width * parts), tokens.dtype)
    full = lax.dynamic_update_slice_in_dim(full, tokens, me * width, 1)
    for shift in range(1, parts):
        ring = [(i, (i + shift) % parts) for i in range(parts)]
        arrived = lax.ppermute(tokens, "fsdp", ring)
        owner = (me - shift + parts) % parts
        full = lax.dynamic_update_slice_in_dim(full, arrived, owner * width, 1)
    return full


def projection_kernel(x_ref, low_ref, w_ref, b_ref, *rest):
    out_ref = rest[-1]
    total = jnp.dot(x_ref[...], w_ref[...], preferred_element_type=jnp.float32)
    total += jnp.dot(low_ref[...], b_ref[...], preferred_element_type=jnp.float32)
    out_ref[...] = total.astype(out_ref.dtype)


def project(x, low_terms, weight, b_terms, start, into=None):
    rows, depth = x.shape
    width, columns = weight.shape[1], b_terms.shape[1]
    block = next(size for size in (512, 256, LANES) if width % size == 0 and start % size == 0)
    if into is not None:
        block = min(block, 2 * LANES)
    first = start // block
    operands = [x, low_terms, weight, b_terms]
    in_specs = [
        pl.BlockSpec(memory_space=pltpu.VMEM),
        pl.BlockSpec(memory_space=pltpu.VMEM),
        pl.BlockSpec((depth, block), lambda i: (0, i)),
        pl.BlockSpec((b_terms.shape[0], block), lambda i: (0, first + i)),
    ]
    aliases = {}
    if into is not None:
        operands.append(into)
        in_specs.append(pl.BlockSpec(memory_space=pl.ANY))
        aliases = {4: 0}
    return pl.pallas_call(
        projection_kernel,
        grid=(width // block,),
        in_specs=in_specs,
        out_specs=pl.BlockSpec((rows, block), lambda i: (0, first + i)),
        out_shape=jax.ShapeDtypeStruct((rows, columns), jnp.bfloat16),
        input_output_aliases=aliases,
        cost_estimate=pl.CostEstimate(
            flops=2 * rows * depth * width,
            bytes_accessed=2 * (depth * width + rows * width),
            transcendentals=0,
        ),
        compiler_params=pltpu.CompilerParams(
            vmem_limit_bytes=40 * 1024 * 1024, dimension_semantics=("arbitrary",)
        ),
    )(*operands)


def three_terms(value):
    terms = []
    for _ in range(3):
        term = lax.reduce_precision(value, 8, 7)
        terms.append(term.astype(jnp.bfloat16))
        value = value - term
    return jnp.concatenate(terms, axis=1)


def per_device(parts, tokens, up_weight, a_bank, b_bank, factor_index, mirror, rewards):
    members_here = mirror.shape[0]
    own_width = members_here * RANK
    position = lax.axis_index("pop")
    flat_index = factor_index.reshape(-1)
    columns = up_weight.shape[1]
    late = max(1, columns // LANES // LATE_SHARE) * LANES
    early = columns - late
    weight_early = lax.all_gather(up_weight[:, :early], "pop", axis=0, tiled=True)
    weight_late = lax.all_gather(up_weight[:, early:], "pop", axis=0, tiled=True)
    piece = whole_rows(tokens, parts)

    picked_a = jnp.take(a_bank, flat_index, axis=0)
    picked_b = jnp.take(b_bank, flat_index, axis=0)
    first_own = position * own_width
    own_a = lax.all_to_all(picked_a, "pop", split_axis=0, concat_axis=1, tiled=True)
    rewards_all, mirror_all = (
        lax.all_gather(rewards, "pop", axis=0, tiled=True),
        lax.all_gather(mirror, "pop", axis=0, tiled=True),
    )
    own_b = lax.dynamic_slice_in_dim(picked_b, first_own, own_width, 0)
    own_signs = (2 * mirror - 1).astype(jnp.float32)
    column_factor = jnp.repeat(noise_scale / math.sqrt(D * RANK) * own_signs, RANK)
    member_of_column = jnp.arange(own_width) // RANK
    row_count = tokens.shape[0]
    low_sum = jnp.dot(piece, own_a.T, preferred_element_type=jnp.float32)
    member_of_row = jnp.arange(row_count) // SEQ
    same_member = member_of_row[:, None] == member_of_column[None, :]
    scaled = jnp.where(same_member, low_sum * column_factor[None, :], 0.0)
    low_terms = three_terms(scaled)
    b_terms = jnp.concatenate([own_b] * 3, axis=0)

    weighting = shaped_weights(rewards_all, mirror_all)
    spread = jnp.repeat(weighting, RANK)
    update = jnp.dot(
        picked_a.astype(jnp.float32).T,
        spread[:, None] * picked_b.astype(jnp.float32),
        precision=lax.Precision.HIGHEST,
    )

    hidden = project(piece, low_terms, weight_early, b_terms, 0)
    hidden = project(piece, low_terms, weight_late, b_terms, early, hidden)
    return (hidden, update)


def solution(mesh):
    parts = mesh.shape["fsdp"]

    def body(*args):
        return per_device(parts, *args)

    in_specs = (
        P("pop", "fsdp"),
        P("pop", "fsdp"),
        P(None, "pop"),
        P(None, "fsdp"),
        P(),
        P("pop"),
        P("pop"),
    )
    out_specs = (P("pop", "fsdp"), P("pop", "fsdp"))
    return jax.shard_map(
        body, mesh=mesh, in_specs=in_specs, out_specs=out_specs, check_vma=False
    )
```
